512 devices in a mesh: client: 4 (over z_hi), expert: 16 (over y, x), shard: 8 (over z_lo, core).
Axes of the slice: x: 4, y: 4, z: 16 (z_hi: 4, z_lo: 4; z = z_hi * 4 + z_lo), core: 2. Of those that a mesh axis runs over, the one named last changes fastest.
Arguments:
- tokens: bfloat16 [4, 2048, 2048], P('client', 'expert'), may hold values from -6 to 6
- target: bfloat16 [4, 2048, 2048], P('client', 'expert'), may hold values from -6 to 6
- routes: int32 [4, 2048, 2], P('client', 'expert'), may hold values from 0 to 7, all different within a row; in each aligned block of 128 rows (0 to 127, 128 to 255, ..., all dimensions but the last counted through in order) at most 32 rows name the same one
- gate_weights: float32 [4, 2048, 2], P('client', 'expert'), may hold values from 0.1 to 1
- counts: int32 [4], replicated, may hold values from 512 to 2048
- gate_proj: bfloat16 [57344, 2048], P(('expert', 'shard'), 'client'), may hold values from -0.125 to 0.125
- up_proj: bfloat16 [57344, 2048], P(('expert', 'shard'), 'client'), may hold values from -0.125 to 0.125
- down_proj: bfloat16 [57344, 2048], P(('expert', 'shard'), 'client'), may hold values from -0.0625 to 0.0625
- correction: bfloat16 [4, 57344, 2048], P('client', ('expert', 'shard')), may hold values from -6 to 6
Outputs:
- pseudo_gradient: float32 [57344, 2048], P(('expert', 'shard'), 'client')
The draws below stay inside these ranges and needn't reach their ends.
Inputs may be any that keep to these rules, and one draw needn't show every extreme that they name: `routes`: in each aligned block of 128 rows of a client, every expert is named by exactly 32 rows; the 2 ids of a row differ.
All inputs are finite; a program needn't handle non-finite values.
Results may differ from the reference program's by a relative error of at most 0.015.
Values may be sent and summed in bfloat16 or wider, within the bound.
No kernel may reach another device: no remote copies, remote signals or barrier semaphores. Data moves between devices by JAX's collectives and lax.ppermute only.
A program may use at most 64 MiB of HBM per device.

```python
import math
import jax
import jax.numpy as jnp
import numpy as np
from jax import lax

D = 2048
FF = 7168
EXPERTS = 8
TOP = 2
LOCAL_STEPS = 2
TOK_DEV = 128
CAP = 32
TOKENS = 2048
CLIENTS = 4
UNITS = 448
N_EXPERT = 16


def touch_ends(values, key, smallest, largest):
    index_at = [jax.random.randint(jax.random.fold_in(key, axis), (), 0, length) for axis, length in enumerate(values.shape)]
    widest = values.shape.index(max(values.shape))
    neighbour = index_at[:widest] + [(index_at[widest] + 1) % values.shape[widest]] + index_at[widest + 1:]
    return values.at[tuple(index_at)].set(smallest).at[tuple(neighbour)].set(largest)


def level_of(rng, dims, cuts, low, high):
    gain = 1.0
    for axis_at, blocks in cuts:
        steps = jax.random.uniform(jax.random.fold_in(jax.random.fold_in(rng, 6), axis_at), (blocks,), jnp.float32, low / len(cuts), high / len(cuts))
        gain = gain * jnp.repeat(jnp.exp(steps), dims[axis_at] // blocks).reshape((-1,) + (1,) * (len(dims) - 1 - axis_at))
    return gain


def shared_out(key, own, number, rows, amount, top, most, lean):
    sequence = jax.random.permutation(key, amount)
    packed, ordinary = load_shares(amount, rows * top, most, lean, True), load_shares(amount, rows * top, most, lean, False)
    places = jnp.arange(amount)

    def named(sizes, offset_by):
        used = int((sizes > 0).sum())
        fixed = max(1, used // 4)
        moved = fixed + (places - fixed + offset_by * (used - fixed)) % max(1, amount - fixed)
        return jnp.zeros((amount,), jnp.int32).at[sequence[jnp.where(places < fixed, places, moved)]].set(jnp.asarray(sizes, jnp.int32))

    sizes = jnp.where(number % 4 == 0, named(packed, number // 4), named(ordinary, number - number // 4 - 1))
    mixed = jax.random.permutation(jax.random.fold_in(own, 3), amount)
    giver, sink = mixed[0:amount // 2 * 2:2], mixed[1:amount // 2 * 2:2]
    room = jnp.minimum(sizes[giver] - 1, most - sizes[sink]) // 2
    room = jnp.where((giver == sequence[0]) | (sink == sequence[0]) | (sizes[sink] == 0), 0, jnp.maximum(room, 0))
    moved = jax.random.randint(jax.random.fold_in(own, 4), (amount // 2,), 0, 1 << 20) % (room + 1)
    sizes = sizes.at[giver].add(-moved).at[sink].add(moved)
    members = jnp.searchsorted(jnp.cumsum(sizes), jnp.arange(rows * top), side="right").astype(jnp.int32)
    table = members.reshape(top, rows).T
    table = table[jax.random.permutation(jax.random.fold_in(own, 1), rows)]
    offset_by = jax.random.randint(jax.random.fold_in(own, 2), (rows, 1), 0, top)
    return jnp.take_along_axis(table, (jnp.arange(top)[None, :] + offset_by) % top, axis=1)


def load_shares(amount, total, most, lean, full):
    weights = [(1 << 20) // math.isqrt(grade ** lean) + 1 for grade in range(1, amount + 1)]
    largest = most if full else min(most, max(-(-total // amount), total * weights[0] // sum(weights)))
    least = 1 if total - largest >= amount - 1 else 0
    given, spare = [largest] + [least] * (amount - 1), total - largest - least * (amount - 1)
    while spare > 0:
        movable = [i for i in range(1, amount) if given[i] < largest] or [i for i in range(1, amount) if given[i] < most]
        pool, left = sum([weights[i] for i in movable]), spare
        for i in movable:
            more = min(most - given[i], max(1, left * weights[i] // pool), spare)
            given[i] = given[i] + more
            spare = spare - more
    return np.array(given)


def gaussian(own_key, extent, deviation, limit, shards=(), kind=jnp.bfloat16):
    factor_of = level_of(own_key, extent, shards, -0.22, 0.18) if shards else 1.0
    drawn = jax.random.normal(own_key, extent, jnp.float32) * deviation * factor_of
    return jnp.minimum(jnp.maximum(drawn, -limit), limit).astype(kind)


def setup_inputs(seed: int = 0) -> dict:
    key_list = jax.random.split(jax.random.key(seed), 10)
    tokens = gaussian(key_list[0], (CLIENTS, TOKENS, D), 1.0, 6.0, ((0, 4), (1, 16)))
    target = gaussian(key_list[1], (CLIENTS, TOKENS, D), 1.0, 6.0, ((0, 4), (1, 16)))
    routes_keys = jax.random.split(jax.random.fold_in(key_list[2], 1), CLIENTS * TOKENS // TOK_DEV)
    routes_turns = jax.random.permutation(jax.random.fold_in(key_list[2], 3), CLIENTS * TOKENS // TOK_DEV)
    routes = jax.vmap(lambda own, number: shared_out(jax.random.fold_in(key_list[2], 2), own, number, TOK_DEV, EXPERTS, TOP, CAP, 2))(routes_keys, routes_turns).reshape((CLIENTS, TOKENS, TOP))
    gate_weights = jnp.clip(0.1 + 0.9 * jax.random.uniform(key_list[3], (CLIENTS, TOKENS, TOP), jnp.float32) ** level_of(key_list[3], (CLIENTS, TOKENS, TOP), ((0, 4), (1, 16)), -0.2, 0.2), 0.1, 1.0)
    counts = touch_ends(jax.random.randint(key_list[4], (CLIENTS,), TOKENS // 4, TOKENS + 1), jax.random.fold_in(key_list[4], 1), TOKENS // 4, TOKENS).astype(jnp.int32)
    gate_proj = gaussian(key_list[5], (EXPERTS * FF, D), D ** -0.5, 0.125, ((0, 128), (1, 4)))
    up_proj = gaussian(key_list[6], (EXPERTS * FF, D), D ** -0.5, 0.125, ((0, 128), (1, 4)))
    down_proj = gaussian(key_list[7], (EXPERTS * FF, D), FF ** -0.5, 0.0625, ((0, 128), (1, 4)))
    correction = gaussian(key_list[8], (CLIENTS, EXPERTS * FF, D), 1.0, 6.0, ((0, 4), (1, 128)))
    return dict(tokens=tokens, target=target, routes=routes, gate_weights=gate_weights, counts=counts, gate_proj=gate_proj, up_proj=up_proj, down_proj=down_proj, correction=correction)


def reference(tokens, target, routes, gate_weights, counts, gate_proj, up_proj, down_proj, correction):
    step_size = 2.0 / FF
    slices = FF // UNITS
    count_total = jnp.sum(counts).astype(jnp.float32)
    contract = (((1,), (1,)), ((), ()))
    result = jnp.zeros((EXPERTS * FF, D), jnp.float32)
    for client in range(CLIENTS):
        features = tokens[client]
        flat_routes = routes[client].reshape(-1)
        gates_flat = gate_weights[client].reshape(-1)
        live_rows = (jnp.arange(TOKENS, dtype=jnp.int32) < counts[client]).astype(jnp.float32)
        goal_rows = target[client].astype(jnp.float32)
        control_shift = correction[client].astype(jnp.float32)
        chosen_list = []
        hidden_list = []
        for expert in range(EXPERTS):
            chosen = jnp.nonzero(flat_routes == expert, size=CAP * N_EXPERT)[0].astype(jnp.int32)
            token_rows = chosen // TOP
            expert_rows = jnp.take(features, token_rows, axis=0)
            gate_block = gate_proj[expert * FF:(expert + 1) * FF]
            up_block = up_proj[expert * FF:(expert + 1) * FF]
            gate_pre = lax.dot_general(expert_rows, gate_block, contract, preferred_element_type=jnp.float32)
            up_pre = lax.dot_general(expert_rows, up_block, contract, preferred_element_type=jnp.float32)
            chosen_list.append(chosen)
            hidden_list.append((jax.nn.silu(gate_pre) * up_pre).astype(jnp.bfloat16))
        iterate = down_proj.astype(jnp.float32)
        grad_sum = jnp.zeros((EXPERTS * FF, D), jnp.float32)
        for step_number in range(LOCAL_STEPS):
            output = jnp.zeros((TOKENS, D), jnp.float32)
            for expert in range(EXPERTS):
                chosen = chosen_list[expert]
                hidden_rows = hidden_list[expert].astype(jnp.float32).reshape(CAP * N_EXPERT, slices, UNITS)
                weight_rows = iterate[expert * FF:(expert + 1) * FF].astype(jnp.bfloat16)
                weight_rows = weight_rows.astype(jnp.float32).reshape(slices, UNITS, D)
                partial_value = jnp.einsum("msu,sud->msd", hidden_rows, weight_rows, precision=lax.Precision.HIGHEST)
                partial_value = lax.optimization_barrier(partial_value.astype(jnp.bfloat16)).astype(jnp.float32)
                row_sum = jnp.sum(partial_value, axis=1)
                weight = jnp.take(gates_flat, chosen, axis=0)
                output = output.at[chosen // TOP].add(weight[:, None] * row_sum)
            residual = live_rows[:, None] * (output - goal_rows)
            gradients = []
            for expert in range(EXPERTS):
                chosen = chosen_list[expert]
                weight = jnp.take(gates_flat, chosen, axis=0)
                cotangent = (weight[:, None] * jnp.take(residual, chosen // TOP, axis=0)).astype(jnp.bfloat16)
                gradients.append(lax.dot_general(hidden_list[expert], cotangent, (((0,), (0,)), ((), ())), preferred_element_type=jnp.float32))
            gradient = jnp.concatenate(gradients, axis=0)
            grad_sum = grad_sum + gradient
            if step_number + 1 < LOCAL_STEPS:
                iterate = iterate - step_size * (gradient + control_shift)
        weight_share = counts[client].astype(jnp.float32) / count_total
        client_term = weight_share * (grad_sum / LOCAL_STEPS + control_shift)
        result = result + lax.optimization_barrier(client_term.astype(jnp.bfloat16)).astype(jnp.float32)
    return result
```

```python
import jax
import jax.numpy as jnp
from jax import lax
from jax.sharding import Mesh, PartitionSpec as P

EXPERTS = 8
LOCAL_STEPS = 2
CORES = 2


F32 = jnp.float32
BF16 = jnp.bfloat16
EXACT = lax.Precision.HIGHEST


def shift(x, axis, by):
    n = lax.axis_size(axis)
    return lax.ppermute(x, axis, [(i, (i + by) % n) for i in range(n)])


def at(x, start, size, axis):
    return lax.dynamic_slice_in_dim(x, start, size, axis)


def dot(a, b, da, db, **kw):
    return lax.dot_general(a, b, (((da,), (db,)), ((), ())), preferred_element_type=F32, **kw)


def ranks(flat):
    n = flat.shape[0]
    onehot = (flat[:, None] == jnp.arange(EXPERTS, dtype=jnp.int32)[None, :]).astype(BF16)
    row = lax.broadcasted_iota(jnp.int32, (n, n), 0)
    col = lax.broadcasted_iota(jnp.int32, (n, n), 1)
    before = dot((col < row).astype(BF16), onehot, 1, 0)
    return jnp.sum(before * onehot.astype(F32), axis=1).astype(jnp.int32)


def place(parts, index_of, axis):
    size = parts[0].shape[axis]
    shape = list(parts[0].shape)
    shape[axis] = size * len(parts)
    out = jnp.zeros(shape, parts[0].dtype)
    for k, part in enumerate(parts):
        out = lax.dynamic_update_slice_in_dim(out, part, index_of(k) * size, axis)
    return out


def local(tokens, target, routes, gate_weights, counts, gate_proj, up_proj, down_proj, correction):
    nc = lax.axis_size("client")
    nm = lax.axis_size("expert")
    nz = lax.axis_size("zlo")
    c = lax.axis_index("client")
    m = lax.axis_index("expert")
    zl = lax.axis_index("zlo")
    q = lax.axis_index("core")
    ns = nz * CORES
    sub = zl * CORES + q
    units, wide = down_proj.shape
    quarter = units // nc
    tok = tokens.shape[1]
    top = routes.shape[2]
    cap = tok * top // EXPERTS
    few = cap // ns
    copies = nm // EXPERTS
    rows = nm * cap
    cols = wide // nz
    pair = nc // CORES
    step_size = 2.0 / (nm * ns * units // EXPERTS)

    def from_client(k):
        return (c - k) % nc

    target_rows = tok * cols // wide
    weights_in, targets_in = [], []
    for k in range(nc):
        to = (c + k) % nc
        goal = at(target[0], (to * nz + zl) * cols, cols, 1).reshape(target_rows, wide)
        block = jnp.concatenate(
            [at(gate_proj, to * quarter, quarter, 0), at(up_proj, to * quarter, quarter, 0), goal], axis=0
        )
        got = shift(block, "client", k) if k else block
        weights_in.append(got[: 2 * quarter])
        targets_in.append(got[2 * quarter :].reshape(tok, cols))
    weights = place(weights_in, from_client, 1)

    flat = routes[0].reshape(-1)
    rank = ranks(flat).reshape(tok, top)
    slot = routes[0] * cap + rank
    wanted = (
        jnp.arange(EXPERTS, dtype=jnp.int32)[:, None] * cap + sub * few + jnp.arange(few, dtype=jnp.int32)[None, :]
    ).reshape(-1)
    pick = jnp.zeros((EXPERTS * few, tok), BF16)
    for k in range(top):
        pick = pick + (slot[None, :, k] == wanted[:, None]).astype(BF16)
    sent = dot(pick, tokens[0], 1, 0).astype(BF16).reshape(EXPERTS, few, -1)
    sent = jnp.repeat(sent, copies, axis=0)
    features = lax.all_to_all(sent, "expert", 0, 0, tiled=True).reshape(nm * few, -1)
    features = lax.all_gather(features, ("client", "zlo", "core"), axis=0, tiled=True)

    pre = dot(weights, features, 1, 1)
    hidden = (jax.nn.silu(pre[:quarter]) * pre[quarter:]).astype(BF16)
    old = lax.broadcasted_iota(jnp.int32, (rows, rows), 0)
    new = lax.broadcasted_iota(jnp.int32, (rows, rows), 1)
    part, src, within = old // (nm * few), old // few % nm, old % few
    order = (src * cap + part * few + within == new).astype(BF16)
    hidden = jnp.concatenate(
        [dot(hidden[:, i * rows : (i + 1) * rows], order, 1, 0).astype(BF16) for i in range(nc)], axis=1
    )
    half = quarter // 2
    right = shift(hidden, "client", 1)
    left = shift(hidden, "client", -1)
    across = jnp.concatenate(
        [shift(right[:half], "client", 1), shift(left[half:], "client", -1)], axis=0
    )
    full = place([hidden, right, across, left], from_client, 0)

    def of_client(i):
        return at(full, i * rows, rows, 1)

    control_in = []
    for k in range(nc):
        block = at(correction[0], (c + k) % nc * wide, wide, 1)
        control_in.append(shift(block, "client", k) if k else block)
    share = counts.astype(F32) / jnp.sum(counts).astype(F32)
    control_sum = sum(share[from_client(k)] * control_in[k].astype(F32) for k in range(nc))

    def over_cores(x):
        keep = at(x, q * (x.shape[0] // CORES), x.shape[0] // CORES, 0)
        give = at(x, (1 - q) * (x.shape[0] // CORES), x.shape[0] // CORES, 0)
        return keep + shift(give.astype(BF16), "core", 1).astype(F32)

    def over_zlo(x, axis):
        size = x.shape[axis] // nz
        total = at(x, zl * size, size, axis)
        low = x.astype(BF16)
        for k in range(1, nz):
            total = total + shift(at(low, (zl + k) % nz * size, size, axis), "zlo", k).astype(F32)
        return total

    first = over_zlo(over_cores(dot(full, down_proj, 0, 0)), 1)

    gram_rows = rows // nc
    gram = jnp.stack([dot(at(of_client(i), c * gram_rows, gram_rows, 1), of_client(i), 0, 0) for i in range(nc)])
    gram = over_zlo(over_cores(gram), 1).astype(BF16)
    gram = lax.all_gather(gram, ("client", "zlo"), axis=1, tiled=True)

    shift_sum = jnp.zeros((nc, rows, wide), F32)
    for k in range(nc):
        i = from_client(k)
        term = dot(of_client(i), control_in[k], 0, 0)
        shift_sum = lax.dynamic_update_slice(shift_sum, term[None], (i, 0, 0))
    shift_sum = over_zlo(over_cores(shift_sum.reshape(nc * rows, wide)), 1)

    table = jnp.concatenate([routes[0].astype(F32), gate_weights[0]], axis=1).T
    table = lax.all_gather(table, "client", axis=0)
    mine = at(table, q * pair, pair, 0)
    goals = jnp.stack(targets_in)
    slots = jnp.arange(EXPERTS * cap, dtype=jnp.int32)
    combine, residual_mask, goal_of, shares = [], [], [], []
    for a in range(pair):
        i = q * pair + a
        chosen = mine[a, :top].T.astype(jnp.int32)
        gates = mine[a, top:].T
        slot_of = chosen * cap + ranks(chosen.reshape(-1)).reshape(tok, top)
        weight = jnp.zeros((tok, EXPERTS * cap), F32)
        for k in range(top):
            weight = weight + jnp.where(slot_of[:, k][:, None] == slots[None, :], gates[:, k][:, None], 0.0)
        combine.append(weight)
        positions = m * tok + jnp.arange(tok, dtype=jnp.int32)
        residual_mask.append((positions < counts[i]).astype(F32)[:, None])
        goal_of.append(lax.dynamic_index_in_dim(goals, (c - i) % nc, 0, keepdims=False).astype(F32))
        shares.append(share[i])

    def at_owner(x):
        x = x.astype(BF16).reshape(pair, nm, cap, cols).transpose(1, 0, 2, 3)
        x = lax.all_to_all(x, "expert", 0, 0, tiled=True).astype(F32)
        x = jnp.sum(x.reshape(EXPERTS, copies, pair, cap, cols), axis=1)
        return [dot(combine[a], x[:, a].reshape(EXPERTS * cap, cols), 1, 0, precision=EXACT) for a in range(pair)]

    def at_expert(x):
        x = jnp.stack(
            [dot(combine[a], x[a], 0, 0, precision=EXACT).astype(BF16).reshape(EXPERTS, cap, cols) for a in range(pair)],
            axis=1,
        )
        x = lax.all_to_all(jnp.repeat(x, copies, axis=0), "expert", 0, 0, tiled=True)
        return x.transpose(1, 0, 2, 3).reshape(pair, rows, cols)

    out = at_owner(first)
    residual = [residual_mask[a] * (out[a] - goal_of[a]) for a in range(pair)]
    cotangent = at_expert(residual)
    change = jnp.concatenate([dot(gram[a], cotangent[a], 1, 0) for a in range(pair)], axis=0) + shift_sum
    moved = at_owner(change)
    mean = [
        shares[a] * (residual[a] - (step_size / LOCAL_STEPS) * residual_mask[a] * moved[a]) for a in range(pair)
    ]
    cotangent = at_expert(mean).reshape(pair * rows, cols)

    chunks = [cotangent] + [shift(cotangent, "zlo", k) for k in range(1, nz)]
    cotangent = place(chunks, lambda k: (zl - k) % nz, 1)
    cotangent = place([cotangent, shift(cotangent, "core", 1)], lambda k: (q + k) % CORES, 0)
    return dot(full, cotangent, 1, 0) + control_sum


def solution(mesh):
    nc, nm, ns = mesh.devices.shape
    grid = Mesh(mesh.devices.reshape(nc, nm, ns // CORES, CORES), ("client", "expert", "zlo", "core"))
    by_token = P("client", "expert", None)
    by_unit = P(("expert", "zlo", "core"), "client")
    return jax.shard_map(
        local,
        mesh=grid,
        in_specs=(
            by_token,
            by_token,
            by_token,
            by_token,
            P(),
            by_unit,
            by_unit,
            by_unit,
            P("client", ("expert", "zlo", "core"), None),
        ),
        out_specs=by_unit,
        check_vma=False,
    )
```

```python
import jax
import jax.numpy as jnp
from jax import lax
from jax.sharding import Mesh, PartitionSpec as P


EXPERTS = 8
LOCAL_STEPS = 2
CORES = 2


F32 = jnp.float32
BF16 = jnp.bfloat16
EXACT = lax.Precision.HIGHEST


def shift(x, axis, by):
    n = lax.axis_size(axis)
    return lax.ppermute(x, axis, [(i, (i + by) % n) for i in range(n)])


def at(x, start, size, axis):
    return lax.dynamic_slice_in_dim(x, start, size, axis)


def dot(a, b, da, db, **kw):
    return lax.dot_general(a, b, (((da,), (db,)), ((), ())), preferred_element_type=F32, **kw)


def ranks(flat):
    n = flat.shape[0]
    onehot = (flat[:, None] == jnp.arange(EXPERTS, dtype=jnp.int32)[None, :]).astype(BF16)
    row = lax.broadcasted_iota(jnp.int32, (n, n), 0)
    col = lax.broadcasted_iota(jnp.int32, (n, n), 1)
    before = dot((col < row).astype(BF16), onehot, 1, 0)
    return jnp.sum(before * onehot.astype(F32), axis=1).astype(jnp.int32)


def place(parts, index_of, axis):
    size = parts[0].shape[axis]
    shape = list(parts[0].shape)
    shape[axis] = size * len(parts)
    out = jnp.zeros(shape, parts[0].dtype)
    for k, part in enumerate(parts):
        out = lax.dynamic_update_slice_in_dim(out, part, index_of(k) * size, axis)
    return out


def local(tokens, target, routes, gate_weights, counts, gate_proj, up_proj, down_proj, correction):
    nc = lax.axis_size("client")
    nm = lax.axis_size("expert")
    nz = lax.axis_size("zlo")
    c = lax.axis_index("client")
    m = lax.axis_index("expert")
    zl = lax.axis_index("zlo")
    q = lax.axis_index("core")
    ns = nz * CORES
    sub = zl * CORES + q
    units, wide = down_proj.shape
    quarter = units // nc
    tok = tokens.shape[1]
    top = routes.shape[2]
    cap = tok * top // EXPERTS
    few = cap // ns
    copies = nm // EXPERTS
    rows = nm * cap
    cols = wide // nz
    pair = nc // CORES
    step_size = 2.0 / (nm * ns * units // EXPERTS)

    def from_client(k):
        return (c - k) % nc

    target_rows = tok * cols // wide
    weights_in, targets_in = [], []
    for k in range(nc):
        to = (c + k) % nc
        goal = at(target[0], (to * nz + zl) * cols, cols, 1).reshape(target_rows, wide)
        block = jnp.concatenate(
            [at(gate_proj, to * quarter, quarter, 0), at(up_proj, to * quarter, quarter, 0), goal], axis=0
        )
        got = shift(block, "client", k) if k else block
        weights_in.append(got[: 2 * quarter])
        targets_in.append(got[2 * quarter :].reshape(tok, cols))
    weights = place(weights_in, from_client, 1)

    flat = routes[0].reshape(-1)
    rank = ranks(flat).reshape(tok, top)
    slot = routes[0] * cap + rank
    wanted = (
        jnp.arange(EXPERTS, dtype=jnp.int32)[:, None] * cap + sub * few + jnp.arange(few, dtype=jnp.int32)[None, :]
    ).reshape(-1)
    pick = jnp.zeros((EXPERTS * few, tok), BF16)
    for k in range(top):
        pick = pick + (slot[None, :, k] == wanted[:, None]).astype(BF16)
    sent = dot(pick, tokens[0], 1, 0).astype(BF16).reshape(EXPERTS, few, -1)
    sent = jnp.repeat(sent, copies, axis=0)
    features = lax.all_to_all(sent, "expert", 0, 0, tiled=True).reshape(nm * few, -1)
    features = lax.all_gather(features, ("client", "zlo", "core"), axis=0, tiled=True)

    pre = dot(weights, features, 1, 1)
    hidden = (jax.nn.silu(pre[:quarter]) * pre[quarter:]).astype(BF16)
    old = lax.broadcasted_iota(jnp.int32, (rows, rows), 0)
    new = lax.broadcasted_iota(jnp.int32, (rows, rows), 1)
    part, src, within = old // (nm * few), old // few % nm, old % few
    order = (src * cap + part * few + within == new).astype(BF16)
    hidden = jnp.concatenate(
        [dot(hidden[:, i * rows : (i + 1) * rows], order, 1, 0).astype(BF16) for i in range(nc)], axis=1
    )
    half = quarter // 2
    right = shift(hidden, "client", 1)
    left = shift(hidden, "client", -1)
    across = jnp.concatenate(
        [shift(right[:half], "client", 1), shift(left[half:], "client", -1)], axis=0
    )
    full = place([hidden, right, across, left], from_client, 0)

    def of_client(i):
        return at(full, i * rows, rows, 1)

    def over_cores(x):
        keep = at(x, q * (x.shape[0] // CORES), x.shape[0] // CORES, 0)
        give = at(x, (1 - q) * (x.shape[0] // CORES), x.shape[0] // CORES, 0)
        return keep + shift(give.astype(BF16), "core", 1).astype(F32)

    def over_zlo(x, axis):
        size = x.shape[axis] // nz
        total = at(x, zl * size, size, axis)
        low = x.astype(BF16)
        for k in range(1, nz):
            total = total + shift(at(low, (zl + k) % nz * size, size, axis), "zlo", k).astype(F32)
        return total

    gram_rows = rows // nc
    value = dot(full, down_proj, 0, 0)
    gram = [dot(at(of_client(i), c * gram_rows, gram_rows, 1), of_client(i), 0, 0) for i in range(nc)]
    both = []
    for p in range(CORES):
        both.append(value[p * pair * rows : (p + 1) * pair * rows])
        both.extend(gram[p * pair : (p + 1) * pair])
    both = over_zlo(over_cores(jnp.concatenate(both, axis=0)), 1).astype(BF16)
    first = both[: pair * rows]
    gram = lax.all_gather(both[pair * rows :], ("client", "zlo"), axis=0, tiled=False)
    gram = gram.reshape(nc, nz, pair, gram_rows, cols).transpose(2, 0, 3, 1, 4).reshape(pair, rows, rows)

    own = of_client(c)
    moved = jnp.concatenate([dot(own, correction[0][:, k * wide : (k + 1) * wide], 0, 0) for k in range(nc)], axis=0)
    moved = over_cores(moved)
    moved, control, _ = lax.optimization_barrier((moved, correction[0], first))
    moved = over_zlo(moved, 1)
    moved = moved.astype(BF16).reshape(CORES, rows, cols)
    odd = c % 2
    arrived = []
    for d in range(2):
        item = lax.dynamic_index_in_dim(moved, odd ^ d, 0, keepdims=False)
        ends = [
            ((2 * p + e) * CORES + r, (2 * r + (e ^ d)) * CORES + p)
            for p in range(CORES)
            for e in range(2)
            for r in range(CORES)
        ]
        arrived.append(lax.ppermute(item, ("client", "core"), ends))
    arrived = jnp.stack(arrived)
    control_move = jnp.concatenate(
        [lax.dynamic_index_in_dim(arrived, odd ^ a, 0, keepdims=False) for a in range(pair)], axis=0
    ).astype(F32)

    share = counts.astype(F32) / jnp.sum(counts).astype(F32)

    def control_to(k):
        return share[c] * at(control, (c + k) % nc * wide, wide, 1).astype(F32)

    mid = units // 2
    far = control_to(2).astype(BF16)
    from_left = shift(far[:mid], "client", 1).astype(F32)
    from_right = shift(far[mid:], "client", -1).astype(F32)
    to_right, to_left = control_to(1), control_to(3)
    to_right = jnp.concatenate([to_right[:mid] + from_left, to_right[mid:]], axis=0).astype(BF16)
    to_left = jnp.concatenate([to_left[:mid], to_left[mid:] + from_right], axis=0).astype(BF16)
    from_left, from_right = shift(to_right, "client", 1), shift(to_left, "client", -1)
    control_sum = control_to(0) + from_left.astype(F32) + from_right.astype(F32)

    table = jnp.concatenate([routes[0].astype(F32), gate_weights[0]], axis=1).T
    tables = jnp.stack([table] + [shift(table, "client", k) for k in range(1, nc)])
    goals = jnp.stack(targets_in)
    slots = jnp.arange(EXPERTS * cap, dtype=jnp.int32)
    combine, residual_mask, goal_of, shares = [], [], [], []
    for a in range(pair):
        i = q * pair + a
        mine = lax.dynamic_index_in_dim(tables, (c - i) % nc, 0, keepdims=False)
        chosen = mine[:top].T.astype(jnp.int32)
        gates = mine[top:].T
        slot_of = chosen * cap + ranks(chosen.reshape(-1)).reshape(tok, top)
        weight = jnp.zeros((tok, EXPERTS * cap), F32)
        for k in range(top):
            weight = weight + jnp.where(slot_of[:, k][:, None] == slots[None, :], gates[:, k][:, None], 0.0)
        combine.append(weight)
        positions = m * tok + jnp.arange(tok, dtype=jnp.int32)
        residual_mask.append((positions < counts[i]).astype(F32)[:, None])
        goal_of.append(lax.dynamic_index_in_dim(goals, (c - i) % nc, 0, keepdims=False).astype(F32))
        shares.append(share[i])

    def at_owner(x):
        x = x.astype(BF16).reshape(pair, nm, cap, cols).transpose(1, 0, 2, 3)
        x = lax.all_to_all(x, "expert", 0, 0, tiled=True)
        x = x.astype(F32)
        x = jnp.sum(x.reshape(EXPERTS, copies, pair, cap, cols), axis=1)
        return [dot(combine[a], x[:, a].reshape(EXPERTS * cap, cols), 1, 0, precision=EXACT) for a in range(pair)]

    def at_expert(x):
        x = jnp.stack(
            [dot(combine[a], x[a], 0, 0, precision=EXACT).astype(BF16).reshape(EXPERTS, cap, cols) for a in range(pair)],
            axis=1,
        )
        x = jnp.repeat(x, copies, axis=0)
        x = lax.all_to_all(x, "expert", 0, 0, tiled=True)
        return x.transpose(1, 0, 2, 3).reshape(pair, rows, cols)

    out = at_owner(first)
    residual = [residual_mask[a] * (out[a] - goal_of[a]) for a in range(pair)]
    cotangent = at_expert(residual)
    change = jnp.concatenate([dot(gram[a], cotangent[a], 1, 0) for a in range(pair)], axis=0) + control_move
    moved = at_owner(change)
    mean = [
        shares[a] * (residual[a] - (step_size / LOCAL_STEPS) * residual_mask[a] * moved[a]) for a in range(pair)
    ]
    cotangent = at_expert(mean).reshape(pair * rows, cols)

    chunks = [cotangent] + [shift(cotangent, "zlo", k) for k in range(1, nz)]
    cotangent = place(chunks, lambda k: (zl - k) % nz, 1)
    cotangent = place([cotangent, shift(cotangent, "core", 1)], lambda k: (q + k) % CORES, 0)
    return dot(full, cotangent, 1, 0) + control_sum


def solution(mesh):
    nc, nm, ns = mesh.devices.shape
    grid = Mesh(mesh.devices.reshape(nc, nm, ns // CORES, CORES), ("client", "expert", "zlo", "core"))
    by_token = P("client", "expert", None)
    by_unit = P(("expert", "zlo", "core"), "client")
    return jax.shard_map(
        local,
        mesh=grid,
        in_specs=(
            by_token,
            by_token,
            by_token,
            by_token,
            P(),
            by_unit,
            by_unit,
            by_unit,
            P("client", ("expert", "zlo", "core"), None),
        ),
        out_specs=by_unit,
        check_vma=False,
    )
```

```python
import jax
import jax.numpy as jnp
from jax import lax
from jax.sharding import Mesh, PartitionSpec as P


EXPERTS = 8
LOCAL_STEPS = 2
CORES = 2


F32 = jnp.float32
BF16 = jnp.bfloat16
EXACT = lax.Precision.HIGHEST


def shift(x, axis, by):
    n = lax.axis_size(axis)
    return lax.ppermute(x, axis, [(i, (i + by) % n) for i in range(n)])


def at(x, start, size, axis):
    return lax.dynamic_slice_in_dim(x, start, size, axis)


def dot(a, b, da, db, **kw):
    return lax.dot_general(a, b, (((da,), (db,)), ((), ())), preferred_element_type=F32, **kw)


def ranks(flat):
    n = flat.shape[0]
    onehot = (flat[:, None] == jnp.arange(EXPERTS, dtype=jnp.int32)[None, :]).astype(BF16)
    row = lax.broadcasted_iota(jnp.int32, (n, n), 0)
    col = lax.broadcasted_iota(jnp.int32, (n, n), 1)
    before = dot((col < row).astype(BF16), onehot, 1, 0)
    return jnp.sum(before * onehot.astype(F32), axis=1).astype(jnp.int32)


def place(parts, index_of, axis):
    size = parts[0].shape[axis]
    shape = list(parts[0].shape)
    shape[axis] = size * len(parts)
    out = jnp.zeros(shape, parts[0].dtype)
    for k, part in enumerate(parts):
        out = lax.dynamic_update_slice_in_dim(out, part, index_of(k) * size, axis)
    return out


def local(tokens, target, routes, gate_weights, counts, gate_proj, up_proj, down_proj, correction):
    nc = lax.axis_size("client")
    nm = lax.axis_size("expert")
    nz = lax.axis_size("zlo")
    c = lax.axis_index("client")
    m = lax.axis_index("expert")
    zl = lax.axis_index("zlo")
    q = lax.axis_index("core")
    ns = nz * CORES
    sub = zl * CORES + q
    units, wide = down_proj.shape
    quarter = units // nc
    tok = tokens.shape[1]
    top = routes.shape[2]
    cap = tok * top // EXPERTS
    few = cap // ns
    copies = nm // EXPERTS
    rows = nm * cap
    cols = wide // nz
    pair = nc // CORES
    step_size = 2.0 / (nm * ns * units // EXPERTS)

    def from_client(k):
        return (c - k) % nc

    weights = []
    for k in range(nc):
        to = (c + k) % nc * quarter
        block = jnp.concatenate([at(gate_proj, to, quarter, 0), at(up_proj, to, quarter, 0)], axis=0)
        weights.append(shift(block, "client", k) if k else block)
    weights = place(weights, from_client, 1)

    flat = routes[0].reshape(-1)
    rank = ranks(flat).reshape(tok, top)
    slot = routes[0] * cap + rank
    wanted = (
        jnp.arange(EXPERTS, dtype=jnp.int32)[:, None] * cap + sub * few + jnp.arange(few, dtype=jnp.int32)[None, :]
    ).reshape(-1)
    pick = jnp.zeros((EXPERTS * few, tok), BF16)
    for k in range(top):
        pick = pick + (slot[None, :, k] == wanted[:, None]).astype(BF16)
    sent = dot(pick, tokens[0], 1, 0).astype(BF16).reshape(EXPERTS, few, -1)
    sent = jnp.repeat(sent, copies, axis=0)
    features = lax.all_to_all(sent, "expert", 0, 0, tiled=True).reshape(nm * few, -1)
    features = lax.all_gather(features, ("client", "zlo", "core"), axis=0, tiled=True)

    pre = dot(weights, features, 1, 1)
    hidden = (jax.nn.silu(pre[:quarter]) * pre[quarter:]).astype(BF16)
    old = lax.broadcasted_iota(jnp.int32, (rows, rows), 0)
    new = lax.broadcasted_iota(jnp.int32, (rows, rows), 1)
    part, src, within = old // (nm * few), old // few % nm, old % few
    order = (src * cap + part * few + within == new).astype(BF16)
    hidden = jnp.concatenate(
        [dot(hidden[:, i * rows : (i + 1) * rows], order, 1, 0).astype(BF16) for i in range(nc)], axis=1
    )
    half = quarter // 2
    top_half, low_half = hidden[:half], hidden[half:]
    right_top = shift(top_half, "client", 1)
    left_low = shift(low_half, "client", -1)
    right_low = shift(low_half, "client", 1)
    left_top = shift(top_half, "client", -1)
    across_top = shift(right_top, "client", 1)
    across_low = shift(left_low, "client", -1)
    full = jnp.zeros((units, nc * rows), BF16)
    for k, upper, lower in ((0, top_half, low_half), (1, right_top, right_low), (2, across_top, across_low), (3, left_top, left_low)):
        full = lax.dynamic_update_slice_in_dim(full, upper, from_client(k) * quarter, 0)
        full = lax.dynamic_update_slice_in_dim(full, lower, from_client(k) * quarter + half, 0)

    def over_zlo(x):
        x = x.astype(BF16).reshape(x.shape[0], nz, x.shape[1] // nz).transpose(1, 0, 2)
        x = lax.all_to_all(x, "zlo", 0, 0, tiled=True)
        return jnp.sum(x.astype(F32), axis=0)

    own = at(full, c * rows, rows, 1)
    some = rows // CORES

    def products(core):
        value = dot(at(full, core * pair * rows, pair * rows, 1), down_proj, 0, 0)
        gram = dot(at(own, core * some, some, 1), own, 0, 0)
        return jnp.concatenate([value, gram], axis=0)

    give = products(1 - q).astype(BF16)
    got = shift(give, "core", 1)
    both = over_zlo(products(q) + got.astype(F32)).astype(BF16)

    def control_products(core):
        first = core * pair * wide
        return jnp.concatenate([dot(own, at(correction[0], first + a * wide, wide, 1), 0, 0) for a in range(pair)], axis=0)

    give = control_products(1 - q).astype(BF16)
    got = shift(give, "core", 1)
    control_move = (control_products(q) + got.astype(F32)).astype(BF16)
    control_move, _ = lax.optimization_barrier((control_move, both))
    totals = at(control_move, zl * cols, cols, 1).astype(F32)
    for k in range(1, nz):
        part = at(control_move, (zl + k) % nz * cols, cols, 1)
        part = shift(part, "zlo", k)
        totals = totals + part.astype(F32)
    control_move = totals

    odd = c % 2

    def hop(x):
        arrived = []
        for d in range(2):
            item = lax.dynamic_index_in_dim(x, odd ^ d, 0, keepdims=False)
            ends = [
                ((2 * p + e) * CORES + r, (2 * r + (e ^ d)) * CORES + p)
                for p in range(CORES)
                for e in range(2)
                for r in range(CORES)
            ]
            arrived.append(lax.ppermute(item, ("client", "core"), ends))
        arrived = jnp.stack(arrived)
        return jnp.stack([lax.dynamic_index_in_dim(arrived, odd ^ a, 0, keepdims=False) for a in range(2)])

    value = hop(both[: pair * rows].reshape(pair, rows, cols))
    value = value.transpose(1, 0, 2).reshape(rows, pair * cols)
    gram = both[pair * rows :]
    gram = [gram] + [shift(gram, "zlo", k) for k in range(1, nz)]
    gram = place(gram, lambda k: (zl - k) % nz, 1)
    other = shift(gram, "core", 1)
    gram = place([gram, other], lambda k: (q + k) % CORES, 0)
    control_move = control_move.reshape(pair, rows, cols).transpose(1, 0, 2).reshape(rows, pair * cols)

    share = counts.astype(F32) / jnp.sum(counts).astype(F32)
    control, _ = lax.optimization_barrier((correction[0], full))

    def control_to(k):
        return share[c] * at(control, (c + k) % nc * wide, wide, 1).astype(F32)

    mid = units // 2
    far = control_to(2).astype(BF16)
    from_left = shift(far[:mid], "client", 1)
    from_right = shift(far[mid:], "client", -1)
    to_right, to_left = control_to(1), control_to(3)
    to_right = jnp.concatenate([to_right[:mid] + from_left.astype(F32), to_right[mid:]], axis=0).astype(BF16)
    to_left = jnp.concatenate([to_left[:mid], to_left[mid:] + from_right.astype(F32)], axis=0).astype(BF16)
    from_left, from_right = shift(to_right, "client", 1), shift(to_left, "client", -1)
    control_sum = control_to(0) + from_left.astype(F32) + from_right.astype(F32)

    slots = jnp.arange(EXPERTS * cap, dtype=jnp.int32)
    combine = jnp.zeros((tok, EXPERTS * cap), F32)
    for k in range(top):
        combine = combine + jnp.where(slot[:, k][:, None] == slots[None, :], gate_weights[0, :, k][:, None], 0.0)
    positions = m * tok + jnp.arange(tok, dtype=jnp.int32)
    live = (positions < counts[c]).astype(F32)[:, None]
    goal = jnp.concatenate(
        [at(target[0], ((q * pair + a) * nz + zl) * cols, cols, 1) for a in range(pair)], axis=1
    ).astype(F32)

    def at_owner(x):
        x = x.astype(BF16).reshape(nm, cap, pair * cols)
        x = lax.all_to_all(x, "expert", 0, 0, tiled=True)
        x = jnp.sum(x.astype(F32).reshape(EXPERTS, copies, cap, pair * cols), axis=1)
        return dot(combine, x.reshape(EXPERTS * cap, pair * cols), 1, 0, precision=EXACT)

    def at_expert(x):
        x = dot(combine, x, 0, 0, precision=EXACT).astype(BF16).reshape(EXPERTS, cap, pair * cols)
        x = jnp.repeat(x, copies, axis=0)
        x = lax.all_to_all(x, "expert", 0, 0, tiled=True)
        return x.reshape(rows, pair * cols)

    residual = live * (at_owner(value) - goal)
    cotangent = at_expert(residual)
    change = dot(gram, cotangent, 1, 0) + control_move
    mean = share[c] * (residual - (step_size / LOCAL_STEPS) * live * at_owner(change))
    cotangent = at_expert(mean)

    cotangent = hop(cotangent.reshape(rows, pair, cols).transpose(1, 0, 2)).reshape(pair * rows, cols)
    cotangent = jnp.broadcast_to(cotangent[None], (nz, pair * rows, cols))
    cotangent = lax.all_to_all(cotangent, "zlo", 0, 0, tiled=True)
    cotangent = cotangent.transpose(1, 0, 2).reshape(pair * rows, wide)
    other = shift(cotangent, "core", 1)
    cotangent = place([cotangent, other], lambda k: (q + k) % CORES, 0)
    return dot(full, cotangent, 1, 0) + control_sum


def solution(mesh):
    nc, nm, ns = mesh.devices.shape
    grid = Mesh(mesh.devices.reshape(nc, nm, ns // CORES, CORES), ("client", "expert", "zlo", "core"))
    by_token = P("client", "expert", None)
    by_unit = P(("expert", "zlo", "core"), "client")
    return jax.shard_map(
        local,
        mesh=grid,
        in_specs=(
            by_token,
            by_token,
            by_token,
            by_token,
            P(),
            by_unit,
            by_unit,
            by_unit,
            P("client", ("expert", "zlo", "core"), None),
        ),
        out_specs=by_unit,
        check_vma=False,
    )
```

```python
import jax
import jax.numpy as jnp
from jax import lax
from jax.sharding import Mesh, PartitionSpec as P


EXPERTS = 8
LOCAL_STEPS = 2
CORES = 2


F32 = jnp.float32
BF16 = jnp.bfloat16
EXACT = lax.Precision.HIGHEST


def shift(x, axis, by):
    n = lax.axis_size(axis)
    return lax.ppermute(x, axis, [(i, (i + by) % n) for i in range(n)])


def at(x, start, size, axis):
    return lax.dynamic_slice_in_dim(x, start, size, axis)


def dot(a, b, da, db, **kw):
    return lax.dot_general(a, b, (((da,), (db,)), ((), ())), preferred_element_type=F32, **kw)


def ranks(flat):
    n = flat.shape[0]
    onehot = (flat[:, None] == jnp.arange(EXPERTS, dtype=jnp.int32)[None, :]).astype(BF16)
    row = lax.broadcasted_iota(jnp.int32, (n, n), 0)
    col = lax.broadcasted_iota(jnp.int32, (n, n), 1)
    before = dot((col < row).astype(BF16), onehot, 1, 0)
    return jnp.sum(before * onehot.astype(F32), axis=1).astype(jnp.int32)


def place(parts, index_of, axis):
    size = parts[0].shape[axis]
    shape = list(parts[0].shape)
    shape[axis] = size * len(parts)
    out = jnp.zeros(shape, parts[0].dtype)
    for k, part in enumerate(parts):
        out = lax.dynamic_update_slice_in_dim(out, part, index_of(k) * size, axis)
    return out


def local(tokens, target, routes, gate_weights, counts, gate_proj, up_proj, down_proj, correction):
    nc = lax.axis_size("client")
    nm = lax.axis_size("expert")
    nz = lax.axis_size("zlo")
    c = lax.axis_index("client")
    m = lax.axis_index("expert")
    zl = lax.axis_index("zlo")
    q = lax.axis_index("core")
    ns = nz * CORES
    sub = zl * CORES + q
    units, wide = down_proj.shape
    quarter = units // nc
    tok = tokens.shape[1]
    top = routes.shape[2]
    cap = tok * top // EXPERTS
    few = cap // ns
    copies = nm // EXPERTS
    rows = nm * cap
    cols = wide // nz
    pair = nc // CORES
    step_size = 2.0 / (nm * ns * units // EXPERTS)

    def from_client(k):
        return (c - k) % nc

    odd = c % 2

    def hop(x):
        arrived = []
        for d in range(2):
            item = lax.dynamic_index_in_dim(x, odd ^ d, 0, keepdims=False)
            ends = [
                ((2 * p + e) * CORES + r, (2 * r + (e ^ d)) * CORES + p)
                for p in range(CORES)
                for e in range(2)
                for r in range(CORES)
            ]
            arrived.append(lax.ppermute(item, ("client", "core"), ends))
        arrived = jnp.stack(arrived)
        return jnp.stack([lax.dynamic_index_in_dim(arrived, odd ^ a, 0, keepdims=False) for a in range(2)])

    weights = []
    for k in range(nc):
        to = (c + k) % nc * quarter
        block = jnp.concatenate([at(gate_proj, to, quarter, 0), at(up_proj, to, quarter, 0)], axis=0)
        weights.append(shift(block, "client", k) if k else block)
    weights = place(weights, from_client, 1)

    flat = routes[0].reshape(-1)
    rank = ranks(flat).reshape(tok, top)
    slot = routes[0] * cap + rank
    wanted = (
        jnp.arange(EXPERTS, dtype=jnp.int32)[:, None] * cap + sub * few + jnp.arange(few, dtype=jnp.int32)[None, :]
    ).reshape(-1)
    pick = jnp.zeros((EXPERTS * few, tok), BF16)
    for k in range(top):
        pick = pick + (slot[None, :, k] == wanted[:, None]).astype(BF16)
    sent = dot(pick, tokens[0], 1, 0).astype(BF16).reshape(EXPERTS, few, -1)
    sent = jnp.repeat(sent, copies, axis=0)
    features = lax.all_to_all(sent, "expert", 0, 0, tiled=True).reshape(nm * few, -1)
    features = lax.all_gather(features, ("client", "zlo", "core"), axis=0, tiled=True)

    pre = dot(weights, features, 1, 1)
    hidden = (jax.nn.silu(pre[:quarter]) * pre[quarter:]).astype(BF16)
    old = lax.broadcasted_iota(jnp.int32, (rows, rows), 0)
    new = lax.broadcasted_iota(jnp.int32, (rows, rows), 1)
    part, src, within = old // (nm * few), old // few % nm, old % few
    order = (src * cap + part * few + within == new).astype(BF16)
    hidden = jnp.concatenate(
        [dot(hidden[:, i * rows : (i + 1) * rows], order, 1, 0).astype(BF16) for i in range(nc)], axis=1
    )
    half = quarter // 2
    top_half, low_half = hidden[:half], hidden[half:]
    right_top = shift(top_half, "client", 1)
    left_low = shift(low_half, "client", -1)
    right_low = shift(low_half, "client", 1)
    left_top = shift(top_half, "client", -1)
    across_top = shift(right_top, "client", 1)
    across_low = shift(left_low, "client", -1)
    full = jnp.zeros((units, nc * rows), BF16)
    for k, upper, lower in ((0, top_half, low_half), (1, right_top, right_low), (2, across_top, across_low), (3, left_top, left_low)):
        full = lax.dynamic_update_slice_in_dim(full, upper, from_client(k) * quarter, 0)
        full = lax.dynamic_update_slice_in_dim(full, lower, from_client(k) * quarter + half, 0)

    def over_zlo(x):
        x = x.astype(BF16).reshape(x.shape[0], nz, x.shape[1] // nz).transpose(1, 0, 2)
        x = lax.all_to_all(x, "zlo", 0, 0, tiled=True)
        return jnp.sum(x.astype(F32), axis=0)

    own = at(full, c * rows, rows, 1)
    some = rows // CORES

    def products(core):
        value = dot(at(full, core * pair * rows, pair * rows, 1), down_proj, 0, 0)
        gram = dot(at(own, core * some, some, 1), own, 0, 0)
        return jnp.concatenate([value, gram], axis=0)

    give = products(1 - q).astype(BF16)
    got = shift(give, "core", 1)
    both = over_zlo(products(q) + got.astype(F32)).astype(BF16)

    control = correction[0].reshape(units, CORES, pair, nz, cols).transpose(0, 3, 1, 2, 4).reshape(units, wide * nc)
    control_move = jnp.concatenate(
        [dot(own, control[:, k * pair * cols : (k + 1) * pair * cols], 0, 0).astype(BF16) for k in range(ns)], axis=0
    )
    control_move = lax.psum_scatter(control_move, ("zlo", "core"), scatter_dimension=0, tiled=True)

    gram = both[pair * rows :]
    gram = [gram] + [shift(gram, "zlo", k) for k in range(1, nz)]
    gram = place(gram, lambda k: (zl - k) % nz, 1)
    other = shift(gram, "core", 1)
    gram = place([gram, other], lambda k: (q + k) % CORES, 0)

    share = counts.astype(F32) / jnp.sum(counts).astype(F32)
    control_sum = (share[c] * correction[0].astype(F32)).astype(BF16).reshape(units, nc, wide).transpose(1, 0, 2)
    control_sum, _ = lax.optimization_barrier((control_sum.reshape(nc * units, wide), both))
    control_sum = lax.psum_scatter(control_sum, "client", scatter_dimension=0, tiled=True)

    slots = jnp.arange(EXPERTS * cap, dtype=jnp.int32)

    def combine_of(slot_of, gates):
        weight = jnp.zeros((tok, EXPERTS * cap), F32)
        for k in range(top):
            weight = weight + jnp.where(slot_of[:, k][:, None] == slots[None, :], gates[:, k][:, None], 0.0)
        return weight

    combine = combine_of(slot, gate_weights[0])
    table = jnp.concatenate([slot.astype(F32), gate_weights[0]], axis=1).T
    tables = hop(jnp.stack([table] * pair))
    combines = [combine_of(tables[a, :top].T.astype(jnp.int32), tables[a, top:].T) for a in range(pair)]
    positions = m * tok + jnp.arange(tok, dtype=jnp.int32)
    live = (positions < counts[c]).astype(F32)[:, None]
    goal = jnp.concatenate(
        [at(target[0], ((q * pair + a) * nz + zl) * cols, cols, 1) for a in range(pair)], axis=1
    ).astype(F32)

    def to_tokens(weight, x):
        x = jnp.sum(x.astype(F32).reshape(EXPERTS, copies, cap, x.shape[-1]), axis=1)
        return dot(weight, x.reshape(EXPERTS * cap, x.shape[-1]), 1, 0, precision=EXACT)

    def to_rows(weight, x):
        return dot(weight, x, 0, 0, precision=EXACT).astype(BF16).reshape(EXPERTS, cap, x.shape[-1])

    def exchange(x):
        return lax.all_to_all(x, "expert", 0, 0, tiled=True)

    value = both[: pair * rows].reshape(pair, nm, cap, cols).transpose(1, 0, 2, 3)
    value = exchange(value)
    value = hop(jnp.stack([to_tokens(combines[a], value[:, a]) for a in range(pair)]).astype(BF16))
    residual = live * (jnp.concatenate([value[a] for a in range(pair)], axis=1).astype(F32) - goal)
    cotangent = exchange(jnp.repeat(to_rows(combine, residual), copies, axis=0))
    cotangent = cotangent.reshape(rows, pair * cols)
    change = dot(gram, cotangent, 1, 0) + control_move.astype(F32)
    change = exchange(change.astype(BF16).reshape(nm, cap, pair * cols))
    mean = share[c] * (residual - (step_size / LOCAL_STEPS) * live * to_tokens(combine, change))
    mean = hop(jnp.stack([mean[:, a * cols : (a + 1) * cols] for a in range(pair)]).astype(BF16))
    cotangent = jnp.stack([to_rows(combines[a], mean[a].astype(F32)) for a in range(pair)], axis=1)
    cotangent = exchange(jnp.repeat(cotangent, copies, axis=0))
    cotangent = cotangent.transpose(1, 0, 2, 3).reshape(pair * rows, cols)

    cotangent = jnp.broadcast_to(cotangent[None], (nz, pair * rows, cols))
    cotangent = lax.all_to_all(cotangent, "zlo", 0, 0, tiled=True)
    cotangent = cotangent.transpose(1, 0, 2).reshape(pair * rows, wide)
    other = shift(cotangent, "core", 1)
    cotangent = place([cotangent, other], lambda k: (q + k) % CORES, 0)
    return dot(full, cotangent, 1, 0) + control_sum.astype(F32)


def solution(mesh):
    nc, nm, ns = mesh.devices.shape
    grid = Mesh(mesh.devices.reshape(nc, nm, ns // CORES, CORES), ("client", "expert", "zlo", "core"))
    by_token = P("client", "expert", None)
    by_unit = P(("expert", "zlo", "core"), "client")
    return jax.shard_map(
        local,
        mesh=grid,
        in_specs=(
            by_token,
            by_token,
            by_token,
            by_token,
            P(),
            by_unit,
            by_unit,
            by_unit,
            P("client", ("expert", "zlo", "core"), None),
        ),
        out_specs=by_unit,
        check_vma=False,
    )
```

```python
import jax
import jax.numpy as jnp
from jax import lax
from jax.sharding import Mesh, PartitionSpec as P


EXPERTS = 8
LOCAL_STEPS = 2
CORES = 2


F32 = jnp.float32
BF16 = jnp.bfloat16
EXACT = lax.Precision.HIGHEST


def shift(x, axis, by):
    n = lax.axis_size(axis)
    return lax.ppermute(x, axis, [(i, (i + by) % n) for i in range(n)])


def at(x, start, size, axis):
    return lax.dynamic_slice_in_dim(x, start, size, axis)


def dot(a, b, da, db, **kw):
    return lax.dot_general(a, b, (((da,), (db,)), ((), ())), preferred_element_type=F32, **kw)


def ranks(flat):
    n = flat.shape[0]
    onehot = (flat[:, None] == jnp.arange(EXPERTS, dtype=jnp.int32)[None, :]).astype(BF16)
    row = lax.broadcasted_iota(jnp.int32, (n, n), 0)
    col = lax.broadcasted_iota(jnp.int32, (n, n), 1)
    before = dot((col < row).astype(BF16), onehot, 1, 0)
    return jnp.sum(before * onehot.astype(F32), axis=1).astype(jnp.int32)


def place(parts, index_of, axis):
    size = parts[0].shape[axis]
    shape = list(parts[0].shape)
    shape[axis] = size * len(parts)
    out = jnp.zeros(shape, parts[0].dtype)
    for k, part in enumerate(parts):
        out = lax.dynamic_update_slice_in_dim(out, part, index_of(k) * size, axis)
    return out


def local(tokens, target, routes, gate_weights, counts, gate_proj, up_proj, down_proj, correction):
    nc = lax.axis_size("client")
    nm = lax.axis_size("expert")
    nz = lax.axis_size("zlo")
    c = lax.axis_index("client")
    m = lax.axis_index("expert")
    zl = lax.axis_index("zlo")
    q = lax.axis_index("core")
    ns = nz * CORES
    sub = zl * CORES + q
    units, wide = down_proj.shape
    quarter = units // nc
    tok = tokens.shape[1]
    top = routes.shape[2]
    cap = tok * top // EXPERTS
    few = cap // ns
    copies = nm // EXPERTS
    rows = nm * cap
    cols = wide // nz
    pair = nc // CORES
    step_size = 2.0 / (nm * ns * units // EXPERTS)

    def from_client(k):
        return (c - k) % nc

    odd = c % 2

    def hop(x):
        arrived = []
        for d in range(2):
            item = lax.dynamic_index_in_dim(x, odd ^ d, 0, keepdims=False)
            ends = [
                ((2 * p + e) * CORES + r, (2 * r + (e ^ d)) * CORES + p)
                for p in range(CORES)
                for e in range(2)
                for r in range(CORES)
            ]
            arrived.append(lax.ppermute(item, ("client", "core"), ends))
        arrived = jnp.stack(arrived)
        return jnp.stack([lax.dynamic_index_in_dim(arrived, odd ^ a, 0, keepdims=False) for a in range(2)])

    weights = []
    for k in range(nc):
        to = (c + k) % nc * quarter
        block = jnp.concatenate([at(gate_proj, to, quarter, 0), at(up_proj, to, quarter, 0)], axis=0)
        weights.append(shift(block, "client", k) if k else block)
    weights = place(weights, from_client, 1)

    flat = routes[0].reshape(-1)
    rank = ranks(flat).reshape(tok, top)
    slot = routes[0] * cap + rank
    wanted = (
        jnp.arange(EXPERTS, dtype=jnp.int32)[:, None] * cap + sub * few + jnp.arange(few, dtype=jnp.int32)[None, :]
    ).reshape(-1)
    pick = jnp.zeros((EXPERTS * few, tok), BF16)
    for k in range(top):
        pick = pick + (slot[None, :, k] == wanted[:, None]).astype(BF16)
    sent = dot(pick, tokens[0], 1, 0).astype(BF16).reshape(EXPERTS, few, -1)
    sent = jnp.repeat(sent, copies, axis=0)
    features = lax.all_to_all(sent, "expert", 0, 0, tiled=True).reshape(nm * few, -1)
    features = lax.all_gather(features, ("client", "zlo", "core"), axis=0, tiled=True)

    slots = jnp.arange(EXPERTS * cap, dtype=jnp.int32)

    def combine_of(slot_of, gates):
        weight = jnp.zeros((tok, EXPERTS * cap), F32)
        for k in range(top):
            weight = weight + jnp.where(slot_of[:, k][:, None] == slots[None, :], gates[:, k][:, None], 0.0)
        return weight

    combine = combine_of(slot, gate_weights[0])
    table = jnp.concatenate([slot.astype(F32), gate_weights[0]], axis=1).T
    tables = hop(jnp.stack([table] * pair))
    combines = [combine_of(tables[a, :top].T.astype(jnp.int32), tables[a, top:].T) for a in range(pair)]
    positions = m * tok + jnp.arange(tok, dtype=jnp.int32)
    live = (positions < counts[c]).astype(F32)[:, None]
    goal = jnp.concatenate(
        [at(target[0], ((q * pair + a) * nz + zl) * cols, cols, 1) for a in range(pair)], axis=1
    ).astype(F32)

    share = counts.astype(F32) / jnp.sum(counts).astype(F32)
    pieces = [
        correction[0][:, ((r * pair + e) * nz + z) * cols : ((r * pair + e) * nz + z + 1) * cols]
        for z in range(nz)
        for r in range(CORES)
        for e in range(pair)
    ]
    control = jnp.concatenate(pieces, axis=1)
    control_sum = jnp.concatenate([correction[0][:, k * wide : (k + 1) * wide] for k in range(nc)], axis=0)
    control_sum = (share[c] * control_sum.astype(F32)).astype(BF16)

    features, control, control_sum, combine, combines, goal = lax.optimization_barrier(
        (features, control, control_sum, combine, combines, goal)
    )

    pre = dot(weights, features, 1, 1)
    hidden = (jax.nn.silu(pre[:quarter]) * pre[quarter:]).astype(BF16)
    old = lax.broadcasted_iota(jnp.int32, (rows, rows), 0)
    new = lax.broadcasted_iota(jnp.int32, (rows, rows), 1)
    part, src, within = old // (nm * few), old // few % nm, old % few
    order = (src * cap + part * few + within == new).astype(BF16)
    hidden = jnp.concatenate(
        [dot(hidden[:, i * rows : (i + 1) * rows], order, 1, 0).astype(BF16) for i in range(nc)], axis=1
    )
    half = quarter // 2
    top_half, low_half = hidden[:half], hidden[half:]
    right_top = shift(top_half, "client", 1)
    left_low = shift(low_half, "client", -1)
    right_low = shift(low_half, "client", 1)
    left_top = shift(top_half, "client", -1)
    across_top = shift(right_top, "client", 1)
    across_low = shift(left_low, "client", -1)
    full = jnp.zeros((units, nc * rows), BF16)
    for k, upper, lower in ((0, top_half, low_half), (1, right_top, right_low), (2, across_top, across_low), (3, left_top, left_low)):
        full = lax.dynamic_update_slice_in_dim(full, upper, from_client(k) * quarter, 0)
        full = lax.dynamic_update_slice_in_dim(full, lower, from_client(k) * quarter + half, 0)

    def over_zlo(x):
        x = x.astype(BF16).reshape(x.shape[0], nz, x.shape[1] // nz).transpose(1, 0, 2)
        x = lax.all_to_all(x, "zlo", 0, 0, tiled=True)
        return jnp.sum(x.astype(F32), axis=0)

    own = at(full, c * rows, rows, 1)
    some = rows // CORES

    def products(core):
        value = dot(at(full, core * pair * rows, pair * rows, 1), down_proj, 0, 0)
        gram = dot(at(own, core * some, some, 1), own, 0, 0)
        return jnp.concatenate([value, gram], axis=0)

    give = products(1 - q).astype(BF16)
    got = shift(give, "core", 1)
    both = over_zlo(products(q) + got.astype(F32)).astype(BF16)

    control_move = dot(own, control, 0, 0).astype(BF16).reshape(rows, ns, pair * cols)
    control_move = control_move.transpose(1, 0, 2).reshape(ns * rows, pair * cols)
    control_move = lax.psum_scatter(control_move, ("zlo", "core"), scatter_dimension=0, tiled=True)

    gram = both[pair * rows :]
    gram = [gram] + [shift(gram, "zlo", k) for k in range(1, nz)]
    gram = place(gram, lambda k: (zl - k) % nz, 1)
    other = shift(gram, "core", 1)
    gram = place([gram, other], lambda k: (q + k) % CORES, 0)

    control_sum, _ = lax.optimization_barrier((control_sum, both))
    control_sum = lax.psum_scatter(control_sum, "client", scatter_dimension=0, tiled=True)

    def to_tokens(weight, x):
        x = jnp.sum(x.astype(F32).reshape(EXPERTS, copies, cap, x.shape[-1]), axis=1)
        return dot(weight, x.reshape(EXPERTS * cap, x.shape[-1]), 1, 0, precision=EXACT)

    def to_rows(weight, x):
        return dot(weight, x, 0, 0, precision=EXACT).astype(BF16).reshape(EXPERTS, cap, x.shape[-1])

    def exchange(x):
        return lax.all_to_all(x, "expert", 0, 0, tiled=True)

    value = both[: pair * rows].reshape(pair, nm, cap, cols).transpose(1, 0, 2, 3)
    value = exchange(value)
    value = hop(jnp.stack([to_tokens(combines[a], value[:, a]) for a in range(pair)]).astype(BF16))
    residual = live * (jnp.concatenate([value[a] for a in range(pair)], axis=1).astype(F32) - goal)
    cotangent = exchange(jnp.repeat(to_rows(combine, residual), copies, axis=0))
    cotangent = cotangent.reshape(rows, pair * cols)
    change = dot(gram, cotangent, 1, 0) + control_move.astype(F32)
    change = exchange(change.astype(BF16).reshape(nm, cap, pair * cols))
    mean = share[c] * (residual - (step_size / LOCAL_STEPS) * live * to_tokens(combine, change))
    mean = hop(jnp.stack([mean[:, a * cols : (a + 1) * cols] for a in range(pair)]).astype(BF16))
    cotangent = jnp.stack([to_rows(combines[a], mean[a].astype(F32)) for a in range(pair)], axis=1)
    cotangent = exchange(jnp.repeat(cotangent, copies, axis=0))
    cotangent = cotangent.transpose(1, 0, 2, 3).reshape(pair * rows, cols)

    cotangent = jnp.broadcast_to(cotangent[None], (nz, pair * rows, cols))
    cotangent = lax.all_to_all(cotangent, "zlo", 0, 0, tiled=True)
    cotangent = cotangent.transpose(1, 0, 2).reshape(pair * rows, wide)
    other = shift(cotangent, "core", 1)
    cotangent = place([cotangent, other], lambda k: (q + k) % CORES, 0)
    return dot(full, cotangent, 1, 0) + control_sum.astype(F32)


def solution(mesh):
    nc, nm, ns = mesh.devices.shape
    grid = Mesh(mesh.devices.reshape(nc, nm, ns // CORES, CORES), ("client", "expert", "zlo", "core"))
    by_token = P("client", "expert", None)
    by_unit = P(("expert", "zlo", "core"), "client")
    return jax.shard_map(
        local,
        mesh=grid,
        in_specs=(
            by_token,
            by_token,
            by_token,
            by_token,
            P(),
            by_unit,
            by_unit,
            by_unit,
            P("client", ("expert", "zlo", "core"), None),
        ),
        out_specs=by_unit,
        check_vma=False,
    )
```

```python
import jax
import jax.numpy as jnp
from jax import lax
from jax.sharding import Mesh, PartitionSpec as P


EXPERTS = 8
LOCAL_STEPS = 2
CORES = 2


F32 = jnp.float32
BF16 = jnp.bfloat16
EXACT = lax.Precision.HIGHEST


def shift(x, axis, by):
    n = lax.axis_size(axis)
    return lax.ppermute(x, axis, [(i, (i + by) % n) for i in range(n)])


def at(x, start, size, axis):
    return lax.dynamic_slice_in_dim(x, start, size, axis)


def dot(a, b, da, db, **kw):
    return lax.dot_general(a, b, (((da,), (db,)), ((), ())), preferred_element_type=F32, **kw)


def ranks(flat):
    n = flat.shape[0]
    onehot = (flat[:, None] == jnp.arange(EXPERTS, dtype=jnp.int32)[None, :]).astype(BF16)
    row = lax.broadcasted_iota(jnp.int32, (n, n), 0)
    col = lax.broadcasted_iota(jnp.int32, (n, n), 1)
    before = dot((col < row).astype(BF16), onehot, 1, 0)
    return jnp.sum(before * onehot.astype(F32), axis=1).astype(jnp.int32)


def place(parts, index_of, axis):
    size = parts[0].shape[axis]
    shape = list(parts[0].shape)
    shape[axis] = size * len(parts)
    out = jnp.zeros(shape, parts[0].dtype)
    for k, part in enumerate(parts):
        out = lax.dynamic_update_slice_in_dim(out, part, index_of(k) * size, axis)
    return out


def local(tokens, target, routes, gate_weights, counts, gate_proj, up_proj, down_proj, correction):
    nc = lax.axis_size("client")
    nm = lax.axis_size("expert")
    nz = lax.axis_size("zlo")
    c = lax.axis_index("client")
    m = lax.axis_index("expert")
    zl = lax.axis_index("zlo")
    q = lax.axis_index("core")
    ns = nz * CORES
    sub = zl * CORES + q
    units, wide = down_proj.shape
    quarter = units // nc
    tok = tokens.shape[1]
    top = routes.shape[2]
    cap = tok * top // EXPERTS
    few = cap // ns
    copies = nm // EXPERTS
    rows = nm * cap
    cols = wide // nz
    pair = nc // CORES
    step_size = 2.0 / (nm * ns * units // EXPERTS)

    def from_client(k):
        return (c - k) % nc

    odd = c % 2

    def hop(x):
        arrived = []
        for d in range(2):
            item = lax.dynamic_index_in_dim(x, odd ^ d, 0, keepdims=False)
            ends = [
                ((2 * p + e) * CORES + r, (2 * r + (e ^ d)) * CORES + p)
                for p in range(CORES)
                for e in range(2)
                for r in range(CORES)
            ]
            arrived.append(lax.ppermute(item, ("client", "core"), ends))
        arrived = jnp.stack(arrived)
        return jnp.stack([lax.dynamic_index_in_dim(arrived, odd ^ a, 0, keepdims=False) for a in range(2)])

    weights = []
    for k in range(nc):
        to = (c + k) % nc * quarter
        block = jnp.concatenate([at(gate_proj, to, quarter, 0), at(up_proj, to, quarter, 0)], axis=0)
        weights.append(shift(block, "client", k) if k else block)
    weights = place(weights, from_client, 1)

    flat = routes[0].reshape(-1)
    rank = ranks(flat).reshape(tok, top)
    slot = routes[0] * cap + rank
    wanted = (
        jnp.arange(EXPERTS, dtype=jnp.int32)[:, None] * cap + sub * few + jnp.arange(few, dtype=jnp.int32)[None, :]
    ).reshape(-1)
    pick = jnp.zeros((EXPERTS * few, tok), BF16)
    for k in range(top):
        pick = pick + (slot[None, :, k] == wanted[:, None]).astype(BF16)
    sent = dot(pick, tokens[0], 1, 0).astype(BF16).reshape(EXPERTS, few, -1)
    sent = jnp.repeat(sent, copies, axis=0)
    features = lax.all_to_all(sent, "expert", 0, 0, tiled=True).reshape(nm * few, -1)
    features = lax.all_gather(features, ("client", "zlo", "core"), axis=0, tiled=True)

    slots = jnp.arange(EXPERTS * cap, dtype=jnp.int32)

    def combine_of(slot_of, gates):
        weight = jnp.zeros((tok, EXPERTS * cap), F32)
        for k in range(top):
            weight = weight + jnp.where(slot_of[:, k][:, None] == slots[None, :], gates[:, k][:, None], 0.0)
        return weight

    combine = combine_of(slot, gate_weights[0])
    table = jnp.concatenate([slot.astype(F32), gate_weights[0]], axis=1).T
    tables = hop(jnp.stack([table] * pair))
    combines = [combine_of(tables[a, :top].T.astype(jnp.int32), tables[a, top:].T) for a in range(pair)]
    positions = m * tok + jnp.arange(tok, dtype=jnp.int32)
    live = (positions < counts[c]).astype(F32)[:, None]
    goal = jnp.concatenate(
        [at(target[0], ((q * pair + a) * nz + zl) * cols, cols, 1) for a in range(pair)], axis=1
    ).astype(F32)

    share = counts.astype(F32) / jnp.sum(counts).astype(F32)
    pieces = [
        correction[0][:, ((r * pair + e) * nz + z) * cols : ((r * pair + e) * nz + z + 1) * cols]
        for z in range(nz)
        for r in range(CORES)
        for e in range(pair)
    ]
    control = jnp.concatenate(pieces, axis=1)
    control_sum = jnp.concatenate([correction[0][:, k * wide : (k + 1) * wide] for k in range(nc)], axis=0)
    control_sum = (share[c] * control_sum.astype(F32)).astype(BF16)

    features, control, control_sum, combine, combines, goal = lax.optimization_barrier(
        (features, control, control_sum, combine, combines, goal)
    )

    pre = dot(weights, features, 1, 1)
    hidden = (jax.nn.silu(pre[:quarter]) * pre[quarter:]).astype(BF16)
    old = lax.broadcasted_iota(jnp.int32, (rows, rows), 0)
    new = lax.broadcasted_iota(jnp.int32, (rows, rows), 1)
    part, src, within = old // (nm * few), old // few % nm, old % few
    order = (src * cap + part * few + within == new).astype(BF16)
    hidden = jnp.concatenate(
        [dot(hidden[:, i * rows : (i + 1) * rows], order, 1, 0).astype(BF16) for i in range(nc)], axis=1
    )
    half = quarter // 2
    top_half, low_half = hidden[:half], hidden[half:]
    right_top = shift(top_half, "client", 1)
    left_low = shift(low_half, "client", -1)
    right_low = shift(low_half, "client", 1)
    left_top = shift(top_half, "client", -1)
    across_top = shift(right_top, "client", 1)
    across_low = shift(left_low, "client", -1)
    full = jnp.zeros((units, nc * rows), BF16)
    for k, upper, lower in ((0, top_half, low_half), (1, right_top, right_low), (2, across_top, across_low), (3, left_top, left_low)):
        full = lax.dynamic_update_slice_in_dim(full, upper, from_client(k) * quarter, 0)
        full = lax.dynamic_update_slice_in_dim(full, lower, from_client(k) * quarter + half, 0)

    def over_zlo(x):
        x = x.astype(BF16).reshape(x.shape[0], nz, x.shape[1] // nz).transpose(1, 0, 2)
        x = lax.all_to_all(x, "zlo", 0, 0, tiled=True)
        return jnp.sum(x.astype(F32), axis=0)

    own = at(full, c * rows, rows, 1)
    some = rows // CORES

    def products(core):
        value = dot(at(full, core * pair * rows, pair * rows, 1), down_proj, 0, 0)
        gram = dot(at(own, core * some, some, 1), own, 0, 0)
        return jnp.concatenate([value, gram], axis=0)

    give = products(1 - q).astype(BF16)
    got = shift(give, "core", 1)
    both = (products(q) + got.astype(F32)).astype(BF16)

    control_move = dot(own, control, 0, 0).astype(BF16).reshape(rows, ns, pair * cols)
    control_move = control_move.transpose(1, 0, 2).reshape(ns * rows, pair * cols)
    control_move = lax.psum_scatter(control_move, ("zlo", "core"), scatter_dimension=0, tiled=True)

    gram = both[pair * rows :].astype(F32)
    for k in range(1, nz):
        part = shift(both[pair * rows :], "zlo", k)
        gram = gram + part.astype(F32)
    gram = gram.astype(BF16)
    other = shift(gram, "core", 1)
    gram = place([gram, other], lambda k: (q + k) % CORES, 0)

    control_sum, _ = lax.optimization_barrier((control_sum, both))
    control_sum = lax.psum_scatter(control_sum, "client", scatter_dimension=0, tiled=True)

    def to_tokens(weight, x):
        x = jnp.sum(x.astype(F32).reshape(EXPERTS, copies, cap, x.shape[-1]), axis=1)
        return dot(weight, x.reshape(EXPERTS * cap, x.shape[-1]), 1, 0, precision=EXACT)

    def to_rows(weight, x):
        return dot(weight, x, 0, 0, precision=EXACT).astype(BF16).reshape(EXPERTS, cap, x.shape[-1])

    def exchange(x):
        return lax.all_to_all(x, "expert", 0, 0, tiled=True)

    value = both[: pair * rows].reshape(pair, nm, cap, wide).transpose(1, 0, 2, 3)
    value = exchange(value)
    value = over_zlo(jnp.concatenate([to_tokens(combines[a], value[:, a]) for a in range(pair)], axis=0))
    value = hop(value.astype(BF16).reshape(pair, tok, cols))
    residual = live * (jnp.concatenate([value[a] for a in range(pair)], axis=1).astype(F32) - goal)
    cotangent = exchange(jnp.repeat(to_rows(combine, residual), copies, axis=0))
    cotangent = cotangent.reshape(rows, pair * cols)
    change = dot(gram, cotangent, 1, 0) + control_move.astype(F32)
    change = exchange(change.astype(BF16).reshape(nm, cap, pair * cols))
    mean = share[c] * (residual - (step_size / LOCAL_STEPS) * live * to_tokens(combine, change))
    mean = hop(jnp.stack([mean[:, a * cols : (a + 1) * cols] for a in range(pair)]).astype(BF16))

    mean = jnp.broadcast_to(mean.reshape(1, pair * tok, cols), (nz, pair * tok, cols))
    mean = lax.all_to_all(mean, "zlo", 0, 0, tiled=True)
    mean = mean.transpose(1, 0, 2).reshape(pair, tok, wide).astype(F32)
    cotangent = jnp.stack([to_rows(combines[a], mean[a]) for a in range(pair)], axis=1)
    cotangent = exchange(jnp.repeat(cotangent, copies, axis=0))
    cotangent = cotangent.transpose(1, 0, 2, 3).reshape(pair * rows, wide)
    other = shift(cotangent, "core", 1)
    cotangent = place([cotangent, other], lambda k: (q + k) % CORES, 0)
    return dot(full, cotangent, 1, 0) + control_sum.astype(F32)


def solution(mesh):
    nc, nm, ns = mesh.devices.shape
    grid = Mesh(mesh.devices.reshape(nc, nm, ns // CORES, CORES), ("client", "expert", "zlo", "core"))
    by_token = P("client", "expert", None)
    by_unit = P(("expert", "zlo", "core"), "client")
    return jax.shard_map(
        local,
        mesh=grid,
        in_specs=(
            by_token,
            by_token,
            by_token,
            by_token,
            P(),
            by_unit,
            by_unit,
            by_unit,
            P("client", ("expert", "zlo", "core"), None),
        ),
        out_specs=by_unit,
        check_vma=False,
    )
```

```python
import jax
import jax.numpy as jnp
from jax import lax
from jax.sharding import Mesh, PartitionSpec as P


EXPERTS = 8
LOCAL_STEPS = 2
CORES = 2


F32 = jnp.float32
BF16 = jnp.bfloat16
EXACT = lax.Precision.HIGHEST


def shift(x, axis, by):
    n = lax.axis_size(axis)
    return lax.ppermute(x, axis, [(i, (i + by) % n) for i in range(n)])


def at(x, start, size, axis):
    return lax.dynamic_slice_in_dim(x, start, size, axis)


def dot(a, b, da, db, **kw):
    return lax.dot_general(a, b, (((da,), (db,)), ((), ())), preferred_element_type=F32, **kw)


def ranks(flat):
    n = flat.shape[0]
    onehot = (flat[:, None] == jnp.arange(EXPERTS, dtype=jnp.int32)[None, :]).astype(BF16)
    row = lax.broadcasted_iota(jnp.int32, (n, n), 0)
    col = lax.broadcasted_iota(jnp.int32, (n, n), 1)
    before = dot((col < row).astype(BF16), onehot, 1, 0)
    return jnp.sum(before * onehot.astype(F32), axis=1).astype(jnp.int32)


def place(parts, index_of, axis):
    size = parts[0].shape[axis]
    shape = list(parts[0].shape)
    shape[axis] = size * len(parts)
    out = jnp.zeros(shape, parts[0].dtype)
    for k, part in enumerate(parts):
        out = lax.dynamic_update_slice_in_dim(out, part, index_of(k) * size, axis)
    return out


def local(tokens, target, routes, gate_weights, counts, gate_proj, up_proj, down_proj, correction):
    nc = lax.axis_size("client")
    nm = lax.axis_size("expert")
    nz = lax.axis_size("zlo")
    c = lax.axis_index("client")
    m = lax.axis_index("expert")
    zl = lax.axis_index("zlo")
    q = lax.axis_index("core")
    ns = nz * CORES
    sub = zl * CORES + q
    units, wide = down_proj.shape
    quarter = units // nc
    tok = tokens.shape[1]
    top = routes.shape[2]
    cap = tok * top // EXPERTS
    few = cap // ns
    copies = nm // EXPERTS
    rows = nm * cap
    cols = wide // nz
    pair = nc // CORES
    step_size = 2.0 / (nm * ns * units // EXPERTS)

    def from_client(k):
        return (c - k) % nc

    odd = c % 2

    def hop(x):
        arrived = []
        for d in range(2):
            item = lax.dynamic_index_in_dim(x, odd ^ d, 0, keepdims=False)
            ends = [
                ((2 * p + e) * CORES + r, (2 * r + (e ^ d)) * CORES + p)
                for p in range(CORES)
                for e in range(2)
                for r in range(CORES)
            ]
            arrived.append(lax.ppermute(item, ("client", "core"), ends))
        arrived = jnp.stack(arrived)
        return jnp.stack([lax.dynamic_index_in_dim(arrived, odd ^ a, 0, keepdims=False) for a in range(2)])

    weights = []
    for k in range(nc):
        to = (c + k) % nc * quarter
        block = jnp.concatenate([at(gate_proj, to, quarter, 0), at(up_proj, to, quarter, 0)], axis=0)
        weights.append(shift(block, "client", k) if k else block)
    weights = place(weights, from_client, 1)

    flat = routes[0].reshape(-1)
    rank = ranks(flat).reshape(tok, top)
    slot = routes[0] * cap + rank
    wanted = (
        jnp.arange(EXPERTS, dtype=jnp.int32)[:, None] * cap + sub * few + jnp.arange(few, dtype=jnp.int32)[None, :]
    ).reshape(-1)
    pick = jnp.zeros((EXPERTS * few, tok), BF16)
    for k in range(top):
        pick = pick + (slot[None, :, k] == wanted[:, None]).astype(BF16)
    sent = dot(pick, tokens[0], 1, 0).astype(BF16).reshape(EXPERTS, few, -1)
    sent = jnp.repeat(sent, copies, axis=0)
    features = lax.all_to_all(sent, "expert", 0, 0, tiled=True).reshape(nm * few, -1)
    features = lax.all_gather(features, ("client", "zlo", "core"), axis=0, tiled=True)

    slots = jnp.arange(EXPERTS * cap, dtype=jnp.int32)

    def combine_of(slot_of, gates):
        weight = jnp.zeros((tok, EXPERTS * cap), F32)
        for k in range(top):
            weight = weight + jnp.where(slot_of[:, k][:, None] == slots[None, :], gates[:, k][:, None], 0.0)
        return weight

    combine = combine_of(slot, gate_weights[0])
    table = jnp.concatenate([slot.astype(F32), gate_weights[0]], axis=1).T
    tables = hop(jnp.stack([table] * pair))
    combines = [combine_of(tables[a, :top].T.astype(jnp.int32), tables[a, top:].T) for a in range(pair)]
    positions = m * tok + jnp.arange(tok, dtype=jnp.int32)
    live = (positions < counts[c]).astype(F32)[:, None]
    goal = jnp.concatenate(
        [at(target[0], ((q * pair + a) * nz + zl) * cols, cols, 1) for a in range(pair)], axis=1
    ).astype(F32)

    share = counts.astype(F32) / jnp.sum(counts).astype(F32)
    pieces = [
        correction[0][:, ((r * pair + e) * nz + z) * cols : ((r * pair + e) * nz + z + 1) * cols]
        for z in range(nz)
        for r in range(CORES)
        for e in range(pair)
    ]
    control = jnp.concatenate(pieces, axis=1)
    control_sum = jnp.concatenate([correction[0][:, k * wide : (k + 1) * wide] for k in range(nc)], axis=0)
    control_sum = (share[c] * control_sum.astype(F32)).astype(BF16)

    features, control, control_sum, combine, combines, goal = lax.optimization_barrier(
        (features, control, control_sum, combine, combines, goal)
    )

    pre = dot(weights, features, 1, 1)
    hidden = (jax.nn.silu(pre[:quarter]) * pre[quarter:]).astype(BF16)
    old = lax.broadcasted_iota(jnp.int32, (rows, rows), 0)
    new = lax.broadcasted_iota(jnp.int32, (rows, rows), 1)
    part, src, within = old // (nm * few), old // few % nm, old % few
    order = (src * cap + part * few + within == new).astype(BF16)
    hidden = jnp.concatenate(
        [dot(hidden[:, i * rows : (i + 1) * rows], order, 1, 0).astype(BF16) for i in range(nc)], axis=1
    )
    half = quarter // 2
    top_half, low_half = hidden[:half], hidden[half:]
    right_top = shift(top_half, "client", 1)
    left_low = shift(low_half, "client", -1)
    right_low = shift(low_half, "client", 1)
    left_top = shift(top_half, "client", -1)
    across_top = shift(right_top, "client", 1)
    across_low = shift(left_low, "client", -1)
    full = jnp.zeros((units, nc * rows), BF16)
    for k, upper, lower in ((0, top_half, low_half), (1, right_top, right_low), (2, across_top, across_low), (3, left_top, left_low)):
        full = lax.dynamic_update_slice_in_dim(full, upper, from_client(k) * quarter, 0)
        full = lax.dynamic_update_slice_in_dim(full, lower, from_client(k) * quarter + half, 0)

    def over_zlo(x):
        x = x.astype(BF16).reshape(x.shape[0], nz, x.shape[1] // nz).transpose(1, 0, 2)
        x = lax.all_to_all(x, "zlo", 0, 0, tiled=True)
        return jnp.sum(x.astype(F32), axis=0)

    own = at(full, c * rows, rows, 1)
    some = rows // CORES

    def products(core):
        value = dot(at(full, core * pair * rows, pair * rows, 1), down_proj, 0, 0)
        gram = dot(at(own, core * some, some, 1), own, 0, 0)
        return jnp.concatenate([value, gram], axis=0)

    give = products(1 - q).astype(BF16)
    got = shift(give, "core", 1)
    both = (products(q) + got.astype(F32)).astype(BF16)

    control_move = dot(own, control, 0, 0).astype(BF16).reshape(rows, ns, pair * cols)
    control_move = control_move.transpose(1, 0, 2).reshape(ns * rows, pair * cols)
    control_move = lax.psum_scatter(control_move, ("zlo", "core"), scatter_dimension=0, tiled=True)

    gram = both[pair * rows :].astype(F32)
    for k in range(1, nz):
        part = shift(both[pair * rows :], "zlo", k)
        gram = gram + part.astype(F32)
    gram = gram.astype(BF16)
    other = shift(gram, "core", 1)
    gram = place([gram, other], lambda k: (q + k) % CORES, 0)

    def control_to(k):
        return at(control_sum, (c + k) % nc * units, units, 0)

    mid = units // 2
    far = control_to(2)
    from_left = shift(far[:mid], "client", 1).astype(F32)
    from_right = shift(far[mid:], "client", -1).astype(F32)
    to_right, to_left = control_to(1), control_to(3)
    to_right = jnp.concatenate([(to_right[:mid].astype(F32) + from_left).astype(BF16), to_right[mid:]], axis=0)
    to_left = jnp.concatenate([to_left[:mid], (to_left[mid:].astype(F32) + from_right).astype(BF16)], axis=0)
    from_left, from_right = shift(to_right, "client", 1), shift(to_left, "client", -1)
    control_sum = control_to(0).astype(F32) + from_left.astype(F32) + from_right.astype(F32)

    def to_tokens(weight, x):
        x = jnp.sum(x.astype(F32).reshape(EXPERTS, copies, cap, x.shape[-1]), axis=1)
        return dot(weight, x.reshape(EXPERTS * cap, x.shape[-1]), 1, 0, precision=EXACT)

    def to_rows(weight, x):
        return dot(weight, x, 0, 0, precision=EXACT).astype(BF16).reshape(EXPERTS, cap, x.shape[-1])

    def exchange(x):
        return lax.all_to_all(x, "expert", 0, 0, tiled=True)

    value = both[: pair * rows].reshape(pair, nm, cap, wide).transpose(1, 0, 2, 3)
    value = exchange(value)
    value = over_zlo(jnp.concatenate([to_tokens(combines[a], value[:, a]) for a in range(pair)], axis=0))
    value = hop(value.astype(BF16).reshape(pair, tok, cols))
    residual = live * (jnp.concatenate([value[a] for a in range(pair)], axis=1).astype(F32) - goal)
    cotangent = exchange(jnp.repeat(to_rows(combine, residual), copies, axis=0))
    cotangent = cotangent.reshape(rows, pair * cols)
    change = dot(gram, cotangent, 1, 0) + control_move.astype(F32)
    change = exchange(change.astype(BF16).reshape(nm, cap, pair * cols))
    mean = share[c] * (residual - (step_size / LOCAL_STEPS) * live * to_tokens(combine, change))
    mean = hop(jnp.stack([mean[:, a * cols : (a + 1) * cols] for a in range(pair)]).astype(BF16))

    mean = jnp.broadcast_to(mean.reshape(1, pair * tok, cols), (nz, pair * tok, cols))
    mean = lax.all_to_all(mean, "zlo", 0, 0, tiled=True)
    mean = mean.transpose(1, 0, 2).reshape(pair, tok, wide).astype(F32)
    cotangent = jnp.stack([to_rows(combines[a], mean[a]) for a in range(pair)], axis=1)
    cotangent = exchange(jnp.repeat(cotangent, copies, axis=0))
    cotangent = cotangent.transpose(1, 0, 2, 3).reshape(pair * rows, wide)
    other = shift(cotangent, "core", 1)
    cotangent = place([cotangent, other], lambda k: (q + k) % CORES, 0)
    return dot(full, cotangent, 1, 0) + control_sum


def solution(mesh):
    nc, nm, ns = mesh.devices.shape
    grid = Mesh(mesh.devices.reshape(nc, nm, ns // CORES, CORES), ("client", "expert", "zlo", "core"))
    by_token = P("client", "expert", None)
    by_unit = P(("expert", "zlo", "core"), "client")
    return jax.shard_map(
        local,
        mesh=grid,
        in_specs=(
            by_token,
            by_token,
            by_token,
            by_token,
            P(),
            by_unit,
            by_unit,
            by_unit,
            P("client", ("expert", "zlo", "core"), None),
        ),
        out_specs=by_unit,
        check_vma=False,
    )
```
